32 devices in a mesh: blk: 8 (over z, y), batch: 4 (over x, core).
Axes of the slice: x: 2, y: 2, z: 4, core: 2. Of those that a mesh axis runs over, the one named last changes fastest.
Arguments:
- coefficients: bfloat16 [120, 24576], P(None, ('blk', 'batch')), may hold values from -6 to 6
- transforms: bfloat16 [12, 24, 24576], P(None, 'batch', 'blk'), may hold values from -6 to 6
- basis: bfloat16 [120, 3, 4096], P(None, None, 'blk'), may hold values from -0.5 to 0.5
- template: bfloat16 [3, 4096], P(None, 'blk'), may hold values from -6 to 6
- skin_weights: bfloat16 [24, 4096], P(None, 'blk'), may hold values from 0.019897461 to 1
Outputs:
- skinned: bfloat16 [24576, 4, 3, 512], P(('blk', 'batch'))
The draws below stay inside these ranges and needn't reach their ends.
All inputs are finite; a program needn't handle non-finite values.
Results may differ from the reference program's by a relative error of at most 0.0049.
Values may be sent and summed in bfloat16 or wider, within the bound.
A program may use at most 192 MiB of HBM per device.

```python
import math
import jax
import jax.numpy as jnp
from jax import lax

K = 120
J = 24
VB = 512
R = 768
STEPS = 4
VERTS = 4096
CHARS = 24576
N_BLK = 8
N_BATCH = 4


def levels(stream_key, dims, pieces, low, top_value):
    def one(axis_at, parts):
        heights = jax.random.uniform(jax.random.fold_in(jax.random.fold_in(stream_key, 6), axis_at), (parts,), jnp.float32, low / len(pieces), top_value / len(pieces))
        return jnp.repeat(jnp.exp(heights), dims[axis_at] // parts).reshape((-1,) + (1,) * (len(dims) - axis_at - 1))

    gain = one(*pieces[0])
    for cut in pieces[1:]:
        gain = gain * one(*cut)
    return gain


def noise(rng, extent, spread, reach, pieces=(), held_as=jnp.bfloat16):
    entries = jax.random.normal(rng, extent, jnp.float32) * spread
    if len(pieces) > 0:
        entries = levels(rng, extent, pieces, -0.22, 0.18) * entries
    return jnp.clip(entries, min=-reach, max=reach).astype(held_as)


def setup_inputs(seed: int = 0) -> dict:
    keys = jax.random.split(jax.random.key(seed), 6)
    return {
        "coefficients": noise(keys[0], (K, CHARS), 1.0, 6.0, ((1, 32),)),
        "transforms": noise(keys[1], (12, J, CHARS), 1.0, 6.0, ((1, 4), (2, 8))),
        "basis": noise(keys[2], (K, 3, VERTS), K ** -0.5, 0.5, ((2, 8),)),
        "template": noise(keys[3], (3, VERTS), 1.0, 6.0, ((1, 8),)),
        "skin_weights": jnp.clip(jnp.exp(math.log(1.0) - 3.9171631 * jax.random.uniform(keys[4], (J, VERTS), jnp.float32) ** levels(keys[4], (J, VERTS), ((1, 8),), -0.2, 0.2)), 0.019897461, 1.0).astype(jnp.bfloat16),
    }


def skin_block(coefficients, joint_poses, basis_block, template_block, weight_block):
    flattened = basis_block.reshape(basis_block.shape[0], -1)
    shaped = jnp.dot(coefficients.T, flattened, preferred_element_type=jnp.float32)
    shaped = shaped + template_block.reshape(1, -1).astype(jnp.float32)
    shaped = shaped.reshape(coefficients.shape[1], 3, -1)
    blended = jnp.einsum("mjr,jv->mrv", joint_poses.astype(jnp.float32), weight_block.astype(jnp.float32))
    positions = []
    for matrix_row in range(3):
        component = blended[4 * matrix_row + 3]
        for column in range(3):
            component = component + blended[4 * matrix_row + column] * shaped[:, column, :]
        positions.append(component)
    return jnp.stack(positions, axis=1).astype(jnp.bfloat16)


def reference(coefficients, transforms, basis, template, skin_weights):
    weight_float = skin_weights.astype(jnp.float32)
    normalized = (weight_float / jnp.sum(weight_float, axis=0, keepdims=True)).astype(jnp.bfloat16)
    group_size = R * N_BATCH

    def per_group(cycle_group):
        offset = (cycle_group * group_size).astype(jnp.int32)
        group_coefficients = lax.dynamic_slice_in_dim(coefficients, offset, group_size, 1)
        group_poses = lax.dynamic_slice_in_dim(transforms, offset, group_size, 2)
        results = []
        for step_index in range(STEPS):
            block_index = jnp.mod(cycle_group - step_index, N_BLK).astype(jnp.int32)
            vertex_offset = (block_index * VB).astype(jnp.int32)
            basis_block = lax.dynamic_slice_in_dim(basis, vertex_offset, VB, 2)
            template_block = lax.dynamic_slice_in_dim(template, vertex_offset, VB, 1)
            weight_block = lax.dynamic_slice_in_dim(normalized, vertex_offset, VB, 1)
            results.append(skin_block(group_coefficients, group_poses, basis_block, template_block, weight_block))
        return jnp.stack(results, axis=1)

    stacked = lax.map(per_group, jnp.arange(N_BLK, dtype=jnp.int32))
    return stacked.reshape(N_BLK * group_size, STEPS, 3, VB)
```

```python
import functools
import jax
import jax.numpy as jnp
from jax import lax
from jax.experimental import pallas as pl
from jax.experimental.pallas import tpu as pltpu
from jax.sharding import PartitionSpec as P

STEPS = 4
LANES = 128
BF16 = jnp.bfloat16
F32 = jnp.float32


def exchange_kernel(
    n_blk, n_batch, tr_ref, ba_ref, te_ref, we_ref,
    tr_out, ba_out, te_out, we_out,
    stage, tr_send, tr_recv, bl_send, bl_recv, fw_send, fw_recv, own_sem,
):
    blk, bat = lax.axis_index("blk"), lax.axis_index("batch")
    sibling = bat + 1 - 2 * lax.rem(bat, 2)
    chars = tr_out.shape[3]
    half = ba_ref.shape[2] // 2
    hop = STEPS - 1

    own = pltpu.make_async_copy(
        tr_ref.at[:, :, pl.ds(pl.multiple_of(bat * chars, LANES), chars)], stage, own_sem.at[0]
    )
    own.start()

    partners = [lax.rem(bat + i, n_batch) for i in range(1, n_batch)]
    ahead = [lax.rem(blk + i, n_blk) for i in range(1, hop + 1)]
    behind = [lax.rem(blk + n_blk - i, n_blk) for i in range(1, hop + 1)]
    barrier = pltpu.get_barrier_semaphore()
    for q in partners:
        pl.semaphore_signal(barrier, inc=1, device_id={"blk": blk, "batch": q})
    for b in ahead + behind:
        pl.semaphore_signal(barrier, inc=1, device_id={"blk": b, "batch": bat})
    pl.semaphore_wait(barrier, len(partners) + 2 * hop)

    mine = pl.ds(pl.multiple_of(lax.rem(bat, 2) * half, LANES), half)
    arrays = ((ba_ref, ba_out), (te_ref, te_out), (we_ref, we_out))

    moves = []
    for i, q in enumerate(partners):
        moves.append(pltpu.make_async_remote_copy(
            src_ref=tr_ref.at[:, :, pl.ds(pl.multiple_of(q * chars, LANES), chars)],
            dst_ref=tr_out.at[bat],
            send_sem=tr_send.at[i], recv_sem=tr_recv.at[i],
            device_id={"blk": blk, "batch": q},
        ))
    blocks = []
    for i, b in enumerate(ahead):
        for k, (src, dst) in enumerate(arrays):
            lead = (slice(None),) * (len(src.shape) - 1)
            blocks.append(pltpu.make_async_remote_copy(
                src_ref=src.at[lead + (mine,)], dst_ref=dst.at[(i,) + lead + (mine,)],
                send_sem=bl_send.at[i, k], recv_sem=bl_recv.at[i, k],
                device_id={"blk": b, "batch": bat},
            ))
    for c in moves + blocks:
        c.start()
    own.wait()
    put = pltpu.make_async_copy(stage, tr_out.at[bat], own_sem.at[1])
    put.start()
    passes = []
    for i in range(hop):
        for k, (src, dst) in enumerate(arrays):
            lead = (i,) + (slice(None),) * (len(src.shape) - 1)
            blocks[3 * i + k].wait_recv()
            c = pltpu.make_async_remote_copy(
                src_ref=dst.at[lead + (mine,)], dst_ref=dst.at[lead + (mine,)],
                send_sem=fw_send.at[i, k], recv_sem=fw_recv.at[i, k],
                device_id={"blk": blk, "batch": sibling},
            )
            c.start()
            passes.append(c)
    put.wait()
    for c in blocks:
        c.wait_send()
    for c in moves + passes:
        c.wait()


def exchange(n_blk, n_batch, transforms, basis, template, weights):
    m, jl, total = transforms.shape
    chars = total // n_batch
    hop = STEPS - 1
    any_spec = pl.BlockSpec(memory_space=pl.ANY)
    dma = pltpu.SemaphoreType.DMA
    return pl.pallas_call(
        functools.partial(exchange_kernel, n_blk, n_batch),
        out_shape=(
            jax.ShapeDtypeStruct((n_batch, m, jl, chars), BF16),
            jax.ShapeDtypeStruct((hop,) + basis.shape, BF16),
            jax.ShapeDtypeStruct((hop,) + template.shape, BF16),
            jax.ShapeDtypeStruct((hop,) + weights.shape, BF16),
        ),
        in_specs=[any_spec] * 4,
        out_specs=(any_spec,) * 4,
        scratch_shapes=[
            pltpu.VMEM((m, jl, chars), BF16),
            dma((n_batch - 1,)), dma((n_batch - 1,)),
            dma((hop, 3)), dma((hop, 3)), dma((hop, 3)), dma((hop, 3)), dma((2,)),
        ],
        compiler_params=pltpu.CompilerParams(
            collective_id=0, has_side_effects=True, vmem_limit_bytes=4 << 20
        ),
        name="exchange",
    )(transforms, basis, template, weights)


def skin_kernel(
    co_ref, tr_ref, ba0_ref, te0_ref, we0_ref, ba_ref, te_ref, we_ref, out_ref,
    basis, weights, mixed, poses, coefs,
):
    rows = co_ref.shape[1]
    k = co_ref.shape[0]
    depth = basis.shape[2]
    comps = poses.shape[0]
    joints = weights.shape[1]
    verts = we0_ref.shape[1]
    tiles = verts // LANES
    wide = 2 * LANES

    @pl.when(pl.program_id(0) == 0)
    def _():
        for s in range(STEPS):
            w = (we0_ref[...] if s == 0 else we_ref[s - 1]).astype(F32)
            weights[s] = (w / jnp.sum(w, axis=0, keepdims=True)).astype(BF16)
            te = te0_ref[...] if s == 0 else te_ref[s - 1]
            for e in range(3):
                basis[s, e, :k] = ba0_ref[e] if s == 0 else ba_ref[s - 1, e]
                row = te[e:e + 1].astype(F32)
                pad = jnp.broadcast_to(row, (depth - k, verts))
                first = lax.broadcasted_iota(jnp.int32, (depth - k, verts), 0) == 0
                basis[s, e, k:] = jnp.where(first, pad, 0.0).astype(BF16)

    ones = jnp.where(
        lax.broadcasted_iota(jnp.int32, (depth - k, rows), 0) == 0, 1.0, 0.0
    ).astype(F32)
    padded = jnp.concatenate([co_ref[...].astype(F32), ones], axis=0)
    coefs[...] = padded.T.astype(BF16)
    for m in range(comps):
        parts = [tr_ref[i, m].astype(F32) for i in range(tr_ref.shape[0])]
        poses[m] = jnp.concatenate(parts, axis=0).T.astype(BF16)

    period = 3 * tiles * STEPS
    for s in range(STEPS):
        for n in range(verts // wide):
            cols = slice(n * wide, (n + 1) * wide)
            w = weights[s, :, cols]
            shaped = [
                jnp.dot(coefs[...], basis[s, e, :, cols], preferred_element_type=F32)
                for e in range(3)
            ]
            for d in range(3):
                total = jnp.dot(poses[4 * d + 3], w, preferred_element_type=F32)
                for e in range(3):
                    total = total + shaped[e] * jnp.dot(
                        poses[4 * d + e], w, preferred_element_type=F32
                    )
                for h in range(wide // LANES):
                    at = (d * tiles + n * (wide // LANES) + h) * STEPS + s
                    mixed[pl.ds(at, rows, stride=period), :] = total[:, h * LANES:(h + 1) * LANES]
    out_ref[...] = mixed[...].astype(BF16)


def skin(coefficients, poses, basis, template, weights, basis_in, template_in, weights_in):
    k, chars = coefficients.shape
    n_batch, comps, jl, _ = poses.shape
    verts = weights.shape[1]
    joints = weights.shape[0]
    rows = LANES
    depth = -(-(k + 1) // 8) * 8
    period = 3 * (verts // LANES) * STEPS

    def whole(a):
        return pl.BlockSpec(a.shape, lambda i: (0,) * a.ndim)

    out = pl.pallas_call(
        skin_kernel,
        grid=(chars // rows,),
        out_shape=jax.ShapeDtypeStruct((chars * period, LANES), BF16),
        in_specs=[
            pl.BlockSpec((k, rows), lambda i: (0, i)),
            pl.BlockSpec((n_batch, comps, jl, rows), lambda i: (0, 0, 0, i)),
            whole(basis), whole(template), whole(weights),
            whole(basis_in), whole(template_in), whole(weights_in),
        ],
        out_specs=pl.BlockSpec((rows * period, LANES), lambda i: (i, 0)),
        scratch_shapes=[
            pltpu.VMEM((STEPS, 3, depth, verts), BF16),
            pltpu.VMEM((STEPS, joints, verts), BF16),
            pltpu.VMEM((rows * period, LANES), F32),
            pltpu.VMEM((comps, rows, joints), BF16),
            pltpu.VMEM((rows, depth), BF16),
        ],
        compiler_params=pltpu.CompilerParams(
            dimension_semantics=("arbitrary",), vmem_limit_bytes=48 << 20
        ),
        name="skin",
    )(coefficients, poses, basis, template, weights, basis_in, template_in, weights_in)
    out = out.reshape(chars, 3, verts // LANES, STEPS, LANES)
    return out.transpose(0, 3, 1, 2, 4).reshape(chars, STEPS, 3, verts)


def solution(mesh):
    n_blk, n_batch = mesh.shape["blk"], mesh.shape["batch"]

    def per_device(coefficients, transforms, basis, template, skin_weights):
        basis = jnp.transpose(basis, (1, 0, 2))
        poses, basis_in, template_in, weights_in = exchange(
            n_blk, n_batch, transforms, basis, template, skin_weights
        )
        return skin(
            coefficients, poses, basis, template, skin_weights,
            basis_in, template_in, weights_in,
        )

    in_specs = (
        P(None, ("blk", "batch")),
        P(None, "batch", "blk"),
        P(None, None, "blk"),
        P(None, "blk"),
        P(None, "blk"),
    )
    out_specs = P(("blk", "batch"), None, None, None)
    return jax.shard_map(
        per_device, mesh=mesh, in_specs=in_specs, out_specs=out_specs, check_vma=False
    )
```

```python
import functools
import jax
import jax.numpy as jnp
from jax import lax
from jax.experimental import pallas as pl
from jax.experimental.pallas import tpu as pltpu
from jax.sharding import PartitionSpec as P

STEPS = 4
LANES = 128
BF16 = jnp.bfloat16
F32 = jnp.float32


def exchange_kernel(
    n_blk, n_batch, tr_ref, ba_ref, te_ref, we_ref,
    tr_out, ba_out, te_out, we_out,
    stage, tr_send, tr_recv, bl_send, bl_recv, fw_send, fw_recv, own_sem,
):
    blk, bat = lax.axis_index("blk"), lax.axis_index("batch")
    sibling = bat + 1 - 2 * lax.rem(bat, 2)
    odd = lax.rem(blk, 2)
    pair = blk + 1 - 2 * odd
    after = lax.rem(blk + 2, n_blk)
    before = lax.rem(blk + n_blk - 2, n_blk)
    chars = tr_out.shape[3]
    half = ba_ref.shape[2] // 2

    own = pltpu.make_async_copy(
        tr_ref.at[:, :, pl.ds(pl.multiple_of(bat * chars, LANES), chars)], stage, own_sem.at[0]
    )
    own.start()

    partners = [lax.rem(bat + i, n_batch) for i in range(1, n_batch)]
    barrier = pltpu.get_barrier_semaphore()
    for q in partners:
        pl.semaphore_signal(barrier, inc=1, device_id={"blk": blk, "batch": q})
    for b in (pair, after, before):
        pl.semaphore_signal(barrier, inc=1, device_id={"blk": b, "batch": bat})
    pl.semaphore_wait(barrier, len(partners) + 3)

    mine = pl.ds(pl.multiple_of(lax.rem(bat, 2) * half, LANES), half)
    arrays = ((ba_ref, ba_out), (te_ref, te_out), (we_ref, we_out))

    def hop(slot_from, slot_to, where, send, recv, target):
        made = []
        for k, (src, dst) in enumerate(arrays):
            lead = (slice(None),) * (len(src.shape) - 1)
            part = src.at[lead + (mine,)] if slot_from == 0 else dst.at[(slot_from - 1,) + lead + (mine,)]
            made.append(pltpu.make_async_remote_copy(
                src_ref=part, dst_ref=dst.at[(slot_to - 1,) + lead + (mine,)],
                send_sem=send.at[where, k], recv_sem=recv.at[slot_to - 1, k],
                device_id={"blk": target[0], "batch": target[1]},
            ))
        return made

    def start(copies):
        for c in copies:
            c.start()

    def arrived(slot):
        for c in hop(slot, slot, slot - 1, bl_send, bl_recv, (pair, bat)):
            c.wait_recv()

    def share(slot):
        start(hop(slot, slot, slot - 1, fw_send, fw_recv, (blk, sibling)))

    start(hop(0, 2, 1, bl_send, bl_recv, (after, bat)))

    @pl.when(odd == 0)
    def _():
        start(hop(0, 1, 0, bl_send, bl_recv, (pair, bat)))

    moves = []
    for i, q in enumerate(partners):
        moves.append(pltpu.make_async_remote_copy(
            src_ref=tr_ref.at[:, :, pl.ds(pl.multiple_of(q * chars, LANES), chars)],
            dst_ref=tr_out.at[bat],
            send_sem=tr_send.at[i], recv_sem=tr_recv.at[i],
            device_id={"blk": blk, "batch": q},
        ))
    start(moves)
    own.wait()
    put = pltpu.make_async_copy(stage, tr_out.at[bat], own_sem.at[1])
    put.start()

    arrived(2)

    @pl.when(odd == 0)
    def _():
        start(hop(2, 3, 2, bl_send, bl_recv, (pair, bat)))

    @pl.when(odd == 1)
    def _():
        start(hop(2, 1, 0, bl_send, bl_recv, (pair, bat)))

    share(2)
    arrived(1)

    @pl.when(odd == 0)
    def _():
        start(hop(1, 3, 3, bl_send, bl_recv, (after, bat)))

    share(1)
    arrived(3)
    share(3)
    put.wait()
    for c in moves:
        c.wait()
    for slot in (2, 1, 3):
        for c in hop(slot, slot, slot - 1, fw_send, fw_recv, (blk, sibling)):
            c.wait()
    for c in hop(0, 2, 1, bl_send, bl_recv, (after, bat)) + hop(0, 1, 0, bl_send, bl_recv, (pair, bat)):
        c.wait_send()

    @pl.when(odd == 0)
    def _():
        for c in hop(2, 3, 2, bl_send, bl_recv, (pair, bat)) + hop(1, 3, 3, bl_send, bl_recv, (after, bat)):
            c.wait_send()


def exchange(n_blk, n_batch, transforms, basis, template, weights):
    m, jl, total = transforms.shape
    chars = total // n_batch
    hop = STEPS - 1
    assert n_blk % 2 == 0 and n_blk > STEPS and n_batch % 2 == 0 and STEPS == 4
    any_spec = pl.BlockSpec(memory_space=pl.ANY)
    hbm_spec = pl.BlockSpec(memory_space=pl.ANY)
    dma = pltpu.SemaphoreType.DMA
    return pl.pallas_call(
        functools.partial(exchange_kernel, n_blk, n_batch),
        out_shape=(
            jax.ShapeDtypeStruct((n_batch, m, jl, chars), BF16),
            jax.ShapeDtypeStruct((hop,) + basis.shape, BF16),
            jax.ShapeDtypeStruct((hop,) + template.shape, BF16),
            jax.ShapeDtypeStruct((hop,) + weights.shape, BF16),
        ),
        in_specs=[hbm_spec] * 4,
        out_specs=(any_spec,) * 4,
        scratch_shapes=[
            pltpu.VMEM((m, jl, chars), BF16),
            dma((n_batch - 1,)), dma((n_batch - 1,)),
            dma((hop + 1, 3)), dma((hop, 3)), dma((hop, 3)), dma((hop, 3)), dma((2,)),
        ],
        compiler_params=pltpu.CompilerParams(
            collective_id=0, has_side_effects=True, vmem_limit_bytes=67043328
        ),
        cost_estimate=pl.CostEstimate(flops=0, bytes_accessed=20 << 20, transcendentals=0),
        name="exchange",
    )(transforms, basis, template, weights)


def skin_kernel(
    co_ref, tr_ref, ba0_ref, te0_ref, we0_ref, ba_ref, te_ref, we_ref, out_ref,
    basis, weights, mixed, poses, coefs,
):
    rows = co_ref.shape[1]
    k = co_ref.shape[0]
    depth = basis.shape[2]
    comps = poses.shape[0]
    joints = weights.shape[1]
    verts = we0_ref.shape[1]
    tiles = verts // LANES
    wide = 2 * LANES

    @pl.when(pl.program_id(0) == 0)
    def _():
        for s in range(STEPS):
            w = (we0_ref[...] if s == 0 else we_ref[s - 1]).astype(F32)
            weights[s] = (w / jnp.sum(w, axis=0, keepdims=True)).astype(BF16)
            te = te0_ref[...] if s == 0 else te_ref[s - 1]
            for e in range(3):
                basis[s, e, :k] = ba0_ref[e] if s == 0 else ba_ref[s - 1, e]
                row = te[e:e + 1].astype(F32)
                pad = jnp.broadcast_to(row, (depth - k, verts))
                first = lax.broadcasted_iota(jnp.int32, (depth - k, verts), 0) == 0
                basis[s, e, k:] = jnp.where(first, pad, 0.0).astype(BF16)

    ones = jnp.where(
        lax.broadcasted_iota(jnp.int32, (depth - k, rows), 0) == 0, 1.0, 0.0
    ).astype(F32)
    padded = jnp.concatenate([co_ref[...].astype(F32), ones], axis=0)
    coefs[...] = padded.T.astype(BF16)
    for m in range(comps):
        parts = [tr_ref[i, m].astype(F32) for i in range(tr_ref.shape[0])]
        poses[m] = jnp.concatenate(parts, axis=0).T.astype(BF16)

    period = 3 * tiles * STEPS
    for s in range(STEPS):
        for n in range(verts // wide):
            cols = slice(n * wide, (n + 1) * wide)
            w = weights[s, :, cols]
            shaped = [
                jnp.dot(coefs[...], basis[s, e, :, cols], preferred_element_type=F32)
                for e in range(3)
            ]
            for d in range(3):
                total = jnp.dot(poses[4 * d + 3], w, preferred_element_type=F32)
                for e in range(3):
                    total = total + shaped[e] * jnp.dot(
                        poses[4 * d + e], w, preferred_element_type=F32
                    )
                for h in range(wide // LANES):
                    at = (d * tiles + n * (wide // LANES) + h) * STEPS + s
                    mixed[pl.ds(at, rows, stride=period), :] = total[:, h * LANES:(h + 1) * LANES]
    out_ref[...] = mixed[...].astype(BF16)


def skin(coefficients, poses, basis, template, weights, basis_in, template_in, weights_in):
    k, chars = coefficients.shape
    n_batch, comps, jl, _ = poses.shape
    verts = weights.shape[1]
    joints = weights.shape[0]
    rows = LANES
    depth = -(-(k + 1) // 8) * 8
    period = 3 * (verts // LANES) * STEPS

    def whole(a):
        return pl.BlockSpec(a.shape, lambda i: (0,) * a.ndim)

    out = pl.pallas_call(
        skin_kernel,
        grid=(chars // rows,),
        out_shape=jax.ShapeDtypeStruct((chars * period, LANES), BF16),
        in_specs=[
            pl.BlockSpec((k, rows), lambda i: (0, i)),
            pl.BlockSpec((n_batch, comps, jl, rows), lambda i: (0, 0, 0, i)),
            whole(basis), whole(template), whole(weights),
            whole(basis_in), whole(template_in), whole(weights_in),
        ],
        out_specs=pl.BlockSpec((rows * period, LANES), lambda i: (i, 0)),
        scratch_shapes=[
            pltpu.VMEM((STEPS, 3, depth, verts), BF16),
            pltpu.VMEM((STEPS, joints, verts), BF16),
            pltpu.VMEM((rows * period, LANES), F32),
            pltpu.VMEM((comps, rows, joints), BF16),
            pltpu.VMEM((rows, depth), BF16),
        ],
        compiler_params=pltpu.CompilerParams(
            dimension_semantics=("arbitrary",), vmem_limit_bytes=67043328
        ),
        name="skin",
    )(coefficients, poses, basis, template, weights, basis_in, template_in, weights_in)
    out = out.reshape(chars, 3, verts // LANES, STEPS, LANES)
    return out.transpose(0, 3, 1, 2, 4).reshape(chars, STEPS, 3, verts)


def solution(mesh):
    n_blk, n_batch = mesh.shape["blk"], mesh.shape["batch"]

    def per_device(coefficients, transforms, basis, template, skin_weights):
        basis = jnp.transpose(basis, (1, 0, 2))
        poses, basis_in, template_in, weights_in = exchange(
            n_blk, n_batch, transforms, basis, template, skin_weights
        )
        return skin(
            coefficients, poses, basis, template, skin_weights,
            basis_in, template_in, weights_in,
        )

    in_specs = (
        P(None, ("blk", "batch")),
        P(None, "batch", "blk"),
        P(None, None, "blk"),
        P(None, "blk"),
        P(None, "blk"),
    )
    out_specs = P(("blk", "batch"), None, None, None)
    return jax.shard_map(
        per_device, mesh=mesh, in_specs=in_specs, out_specs=out_specs, check_vma=False
    )
```

```python
import functools
import jax
import jax.numpy as jnp
from jax import lax
from jax.experimental import pallas as pl
from jax.experimental.pallas import tpu as pltpu
from jax.sharding import PartitionSpec as P

STEPS = 4
LANES = 128
BF16 = jnp.bfloat16
F32 = jnp.float32


def exchange_kernel(
    n_blk, n_batch, tr_ref, ba_ref, te_ref, we_ref,
    tr_out, ba_out, te_out, we_out,
    stage, tr_send, tr_recv, bl_send, bl_recv, fw_send, fw_recv, own_sem,
):
    blk, bat = lax.axis_index("blk"), lax.axis_index("batch")
    sibling = bat + 1 - 2 * lax.rem(bat, 2)
    odd = lax.rem(blk, 2)
    pair = blk + 1 - 2 * odd
    after = lax.rem(blk + 2, n_blk)
    before = lax.rem(blk + n_blk - 2, n_blk)
    chars = tr_out.shape[3]
    half = ba_ref.shape[2] // 2

    own = pltpu.make_async_copy(
        tr_ref.at[:, :, pl.ds(pl.multiple_of(bat * chars, LANES), chars)], stage, own_sem.at[0]
    )
    own.start()

    partners = [lax.rem(bat + i, n_batch) for i in range(1, n_batch)]
    barrier = pltpu.get_barrier_semaphore()
    for q in partners:
        pl.semaphore_signal(barrier, inc=1, device_id={"blk": blk, "batch": q})
    for b in (pair, after, before):
        pl.semaphore_signal(barrier, inc=1, device_id={"blk": b, "batch": bat})
    pl.semaphore_wait(barrier, len(partners) + 3)

    mine = pl.ds(pl.multiple_of(lax.rem(bat, 2) * half, LANES), half)
    pieces = [((te_ref, te_out), (we_ref, we_out), (ba_ref.at[0], ba_out.at[:, 0]))]
    pieces += [((ba_ref.at[e], ba_out.at[:, e]),) for e in range(1, ba_ref.shape[0])]

    def hop(slot_from, slot_to, piece, where, send, recv, target):
        made = []
        for k, (src, dst) in enumerate(pieces[piece]):
            at = piece + k if piece == 0 else piece + 2
            lead = (slice(None),) * (len(src.shape) - 1)
            part = src.at[lead + (mine,)] if slot_from == 0 else dst.at[(slot_from - 1,) + lead + (mine,)]
            made.append(pltpu.make_async_remote_copy(
                src_ref=part, dst_ref=dst.at[(slot_to - 1,) + lead + (mine,)],
                send_sem=send.at[where, at], recv_sem=recv.at[slot_to - 1, at],
                device_id={"blk": target[0], "batch": target[1]},
            ))
        return made

    def start(copies):
        for c in copies:
            c.start()

    def first_hop(piece):
        return hop(0, 2, piece, 1, bl_send, bl_recv, (after, bat))

    def to_odd(piece):
        return hop(0, 1, piece, 0, bl_send, bl_recv, (pair, bat))

    def odd_forward(piece):
        return hop(2, 1, piece, 0, bl_send, bl_recv, (pair, bat))

    def even_forward(piece):
        return hop(2, 3, piece, 2, bl_send, bl_recv, (pair, bat))

    def even_onward(piece):
        return hop(1, 3, piece, 3, bl_send, bl_recv, (after, bat))

    def share(slot, piece):
        return hop(slot, slot, piece, slot - 1, fw_send, fw_recv, (blk, sibling))

    def take(slot, piece):
        for c in hop(slot, slot, piece, slot - 1, bl_send, bl_recv, (pair, bat)):
            c.wait_recv()
        if slot == 2:
            @pl.when(odd == 0)
            def _():
                start(even_forward(piece))

            @pl.when(odd == 1)
            def _():
                start(odd_forward(piece))
        if slot == 1:
            @pl.when(odd == 0)
            def _():
                start(even_onward(piece))
        start(share(slot, piece))

    count = len(pieces)
    for p in range(count):
        start(first_hop(p))

    moves = []
    for i, q in enumerate(partners):
        moves.append(pltpu.make_async_remote_copy(
            src_ref=tr_ref.at[:, :, pl.ds(pl.multiple_of(q * chars, LANES), chars)],
            dst_ref=tr_out.at[bat],
            send_sem=tr_send.at[i], recv_sem=tr_recv.at[i],
            device_id={"blk": blk, "batch": q},
        ))
    start(moves)

    @pl.when(odd == 0)
    def _():
        for p in range(count):
            start(to_odd(p))

    own.wait()
    put = pltpu.make_async_copy(stage, tr_out.at[bat], own_sem.at[1])
    put.start()

    for step in range(count + 2):
        for slot, late in ((2, 0), (1, 1), (3, 2)):
            if 0 <= step - late < count:
                take(slot, step - late)

    put.wait()
    for c in moves:
        c.wait()
    for p in range(count):
        for slot in (2, 1, 3):
            for c in share(slot, p):
                c.wait()
        for c in first_hop(p) + to_odd(p):
            c.wait_send()

        @pl.when(odd == 0)
        def _():
            for c in even_forward(p) + even_onward(p):
                c.wait_send()


def exchange(n_blk, n_batch, transforms, basis, template, weights):
    m, jl, total = transforms.shape
    chars = total // n_batch
    hop = STEPS - 1
    assert n_blk % 2 == 0 and n_blk > STEPS and n_batch % 2 == 0 and STEPS == 4
    any_spec = pl.BlockSpec(memory_space=pl.ANY)
    hbm_spec = pl.BlockSpec(memory_space=pl.ANY)
    dma = pltpu.SemaphoreType.DMA
    return pl.pallas_call(
        functools.partial(exchange_kernel, n_blk, n_batch),
        out_shape=(
            jax.ShapeDtypeStruct((n_batch, m, jl, chars), BF16),
            jax.ShapeDtypeStruct((hop,) + basis.shape, BF16),
            jax.ShapeDtypeStruct((hop,) + template.shape, BF16),
            jax.ShapeDtypeStruct((hop,) + weights.shape, BF16),
        ),
        in_specs=[hbm_spec] * 4,
        out_specs=(any_spec,) * 4,
        scratch_shapes=[
            pltpu.VMEM((m, jl, chars), BF16),
            dma((n_batch - 1,)), dma((n_batch - 1,)),
            dma((hop + 1, 5)), dma((hop, 5)), dma((hop, 5)), dma((hop, 5)), dma((2,)),
        ],
        compiler_params=pltpu.CompilerParams(
            collective_id=0, has_side_effects=True, vmem_limit_bytes=67043328
        ),
        cost_estimate=pl.CostEstimate(flops=0, bytes_accessed=20 << 20, transcendentals=0),
        name="exchange",
    )(transforms, basis, template, weights)


def skin_kernel(
    co_ref, tr_ref, ba0_ref, te0_ref, we0_ref, ba_ref, te_ref, we_ref, out_ref,
    basis, weights, mixed0, mixed1, mixed2, shaped, poses, coefs,
):
    rows = co_ref.shape[1]
    k = co_ref.shape[0]
    depth = basis.shape[2]
    comps = poses.shape[0]
    joints = weights.shape[1]
    verts = we0_ref.shape[1]
    tiles = verts // LANES
    wide = 2 * LANES

    @pl.when(pl.program_id(0) == 0)
    def _():
        for s in range(STEPS):
            w = (we0_ref[...] if s == 0 else we_ref[s - 1]).astype(F32)
            weights[s] = (w / jnp.sum(w, axis=0, keepdims=True)).astype(BF16)
            te = te0_ref[...] if s == 0 else te_ref[s - 1]
            for e in range(3):
                basis[s, e, :k] = ba0_ref[e] if s == 0 else ba_ref[s - 1, e]
                row = te[e:e + 1].astype(F32)
                pad = jnp.broadcast_to(row, (depth - k, verts))
                first = lax.broadcasted_iota(jnp.int32, (depth - k, verts), 0) == 0
                basis[s, e, k:] = jnp.where(first, pad, 0.0).astype(BF16)

    ones = jnp.where(
        lax.broadcasted_iota(jnp.int32, (depth - k, rows), 0) == 0, 1.0, 0.0
    ).astype(F32)
    padded = jnp.concatenate([co_ref[...].astype(F32), ones], axis=0)
    coefs[...] = padded.T.astype(BF16)
    for m in range(comps):
        parts = [tr_ref[i, m].astype(F32) for i in range(tr_ref.shape[0])]
        poses[m] = jnp.concatenate(parts, axis=0).T.astype(BF16)

    group = tiles * STEPS
    halves = verts // wide
    for s in range(STEPS):
        for n in range(halves):
            for e in range(3):
                shaped[s, n, e] = jnp.dot(
                    coefs[...], basis[s, e, :, n * wide:(n + 1) * wide],
                    preferred_element_type=F32,
                )
    for d, mixed in enumerate((mixed0, mixed1, mixed2)):
        for s in range(STEPS):
            for n in range(halves):
                w = weights[s, :, n * wide:(n + 1) * wide]
                total = jnp.dot(poses[4 * d + 3], w, preferred_element_type=F32)
                for e in range(3):
                    total = total + shaped[s, n, e] * jnp.dot(
                        poses[4 * d + e], w, preferred_element_type=F32
                    )
                for h in range(wide // LANES):
                    at = (n * (wide // LANES) + h) * STEPS + s
                    mixed[pl.ds(at, rows, stride=group), :] = total[:, h * LANES:(h + 1) * LANES]
        out_ref[:, d] = mixed[...].reshape(rows, group, LANES).astype(BF16)


def skin(coefficients, poses, basis, template, weights, basis_in, template_in, weights_in):
    k, chars = coefficients.shape
    n_batch, comps, jl, _ = poses.shape
    verts = weights.shape[1]
    joints = weights.shape[0]
    rows = LANES
    depth = -(-(k + 1) // 8) * 8
    group = (verts // LANES) * STEPS

    def whole(a):
        return pl.BlockSpec(a.shape, lambda i: (0,) * a.ndim)

    out = pl.pallas_call(
        skin_kernel,
        grid=(chars // rows,),
        out_shape=jax.ShapeDtypeStruct((chars, 3, group, LANES), BF16),
        in_specs=[
            pl.BlockSpec((k, rows), lambda i: (0, i)),
            pl.BlockSpec((n_batch, comps, jl, rows), lambda i: (0, 0, 0, i)),
            whole(basis), whole(template), whole(weights),
            whole(basis_in), whole(template_in), whole(weights_in),
        ],
        out_specs=pl.BlockSpec((rows, 3, group, LANES), lambda i: (i, 0, 0, 0)),
        scratch_shapes=[
            pltpu.VMEM((STEPS, 3, depth, verts), BF16),
            pltpu.VMEM((STEPS, joints, verts), BF16),
            pltpu.VMEM((rows * group, LANES), F32),
            pltpu.VMEM((rows * group, LANES), F32),
            pltpu.VMEM((rows * group, LANES), F32),
            pltpu.VMEM((STEPS, verts // (2 * LANES), 3, rows, 2 * LANES), F32),
            pltpu.VMEM((comps, rows, joints), BF16),
            pltpu.VMEM((rows, depth), BF16),
        ],
        compiler_params=pltpu.CompilerParams(
            dimension_semantics=("arbitrary",), vmem_limit_bytes=67043328
        ),
        name="skin",
    )(coefficients, poses, basis, template, weights, basis_in, template_in, weights_in)
    out = out.reshape(chars, 3, verts // LANES, STEPS, LANES)
    return out.transpose(0, 3, 1, 2, 4).reshape(chars, STEPS, 3, verts)


def solution(mesh):
    n_blk, n_batch = mesh.shape["blk"], mesh.shape["batch"]

    def per_device(coefficients, transforms, basis, template, skin_weights):
        basis = jnp.transpose(basis, (1, 0, 2))
        poses, basis_in, template_in, weights_in = exchange(
            n_blk, n_batch, transforms, basis, template, skin_weights
        )
        return skin(
            coefficients, poses, basis, template, skin_weights,
            basis_in, template_in, weights_in,
        )

    in_specs = (
        P(None, ("blk", "batch")),
        P(None, "batch", "blk"),
        P(None, None, "blk"),
        P(None, "blk"),
        P(None, "blk"),
    )
    out_specs = P(("blk", "batch"), None, None, None)
    return jax.shard_map(
        per_device, mesh=mesh, in_specs=in_specs, out_specs=out_specs, check_vma=False
    )
```

```python
import functools
import jax
import jax.numpy as jnp
from jax import lax
from jax.experimental import pallas as pl
from jax.experimental.pallas import tpu as pltpu
from jax.sharding import PartitionSpec as P

STEPS = 4
LANES = 128
BF16 = jnp.bfloat16
F32 = jnp.float32


def exchange_kernel(
    n_blk, n_batch, tr_ref, ba_ref, te_ref, we_ref,
    tr_out, ba_out, te_out, we_out,
    stage, tr_send, tr_recv, bl_send, bl_recv, fw_send, fw_recv, own_sem,
):
    blk, bat = lax.axis_index("blk"), lax.axis_index("batch")
    sibling = bat + 1 - 2 * lax.rem(bat, 2)
    odd = lax.rem(blk, 2)
    pair = blk + 1 - 2 * odd
    after = lax.rem(blk + 2, n_blk)
    before = lax.rem(blk + n_blk - 2, n_blk)
    chars = tr_out.shape[3]
    half = ba_ref.shape[2] // 2

    own = pltpu.make_async_copy(
        tr_ref.at[:, :, pl.ds(pl.multiple_of(bat * chars, LANES), chars)], stage, own_sem.at[0]
    )
    own.start()

    partners = [lax.rem(bat + i, n_batch) for i in range(1, n_batch)]
    barrier = pltpu.get_barrier_semaphore()
    for q in partners:
        pl.semaphore_signal(barrier, inc=1, device_id={"blk": blk, "batch": q})
    for b in (pair, after, before):
        pl.semaphore_signal(barrier, inc=1, device_id={"blk": b, "batch": bat})
    pl.semaphore_wait(barrier, len(partners) + 3)

    mine = pl.ds(pl.multiple_of(lax.rem(bat, 2) * half, LANES), half)
    pieces = [((te_ref, te_out), (we_ref, we_out), (ba_ref.at[0], ba_out.at[:, 0]))]
    pieces += [((ba_ref.at[e], ba_out.at[:, e]),) for e in range(1, ba_ref.shape[0])]

    def hop(slot_from, slot_to, piece, where, send, recv, target):
        made = []
        for k, (src, dst) in enumerate(pieces[piece]):
            at = piece + k if piece == 0 else piece + 2
            lead = (slice(None),) * (len(src.shape) - 1)
            part = src.at[lead + (mine,)] if slot_from == 0 else dst.at[(slot_from - 1,) + lead + (mine,)]
            made.append(pltpu.make_async_remote_copy(
                src_ref=part, dst_ref=dst.at[(slot_to - 1,) + lead + (mine,)],
                send_sem=send.at[where, at], recv_sem=recv.at[slot_to - 1, at],
                device_id={"blk": target[0], "batch": target[1]},
            ))
        return made

    def start(copies):
        for c in copies:
            c.start()

    def first_hop(piece):
        return hop(0, 2, piece, 1, bl_send, bl_recv, (after, bat))

    def to_odd(piece):
        return hop(0, 1, piece, 0, bl_send, bl_recv, (pair, bat))

    def odd_forward(piece):
        return hop(2, 1, piece, 0, bl_send, bl_recv, (pair, bat))

    def even_forward(piece):
        return hop(2, 3, piece, 2, bl_send, bl_recv, (pair, bat))

    def even_onward(piece):
        return hop(1, 3, piece, 3, bl_send, bl_recv, (after, bat))

    def share(slot, piece):
        return hop(slot, slot, piece, slot - 1, fw_send, fw_recv, (blk, sibling))

    def take(slot, piece):
        for c in hop(slot, slot, piece, slot - 1, bl_send, bl_recv, (pair, bat)):
            c.wait_recv()
        if slot == 2:
            @pl.when(odd == 0)
            def _():
                start(even_forward(piece))

            @pl.when(odd == 1)
            def _():
                start(odd_forward(piece))
        if slot == 1:
            @pl.when(odd == 0)
            def _():
                start(even_onward(piece))
        start(share(slot, piece))

    count = len(pieces)
    for p in range(count):
        start(first_hop(p))

    moves = []
    for i, q in enumerate(partners):
        moves.append(pltpu.make_async_remote_copy(
            src_ref=tr_ref.at[:, :, pl.ds(pl.multiple_of(q * chars, LANES), chars)],
            dst_ref=tr_out.at[bat],
            send_sem=tr_send.at[i], recv_sem=tr_recv.at[i],
            device_id={"blk": blk, "batch": q},
        ))
    start(moves)

    @pl.when(odd == 0)
    def _():
        for p in range(count):
            start(to_odd(p))

    own.wait()
    put = pltpu.make_async_copy(stage, tr_out.at[bat], own_sem.at[1])
    put.start()

    for step in range(count + 2):
        for slot, late in ((2, 0), (1, 1), (3, 2)):
            if 0 <= step - late < count:
                take(slot, step - late)

    put.wait()
    for c in moves:
        c.wait()
    for p in range(count):
        for slot in (2, 1, 3):
            for c in share(slot, p):
                c.wait()
        for c in first_hop(p) + to_odd(p):
            c.wait_send()

        @pl.when(odd == 0)
        def _():
            for c in even_forward(p) + even_onward(p):
                c.wait_send()


def exchange(n_blk, n_batch, transforms, basis, template, weights):
    m, jl, total = transforms.shape
    chars = total // n_batch
    hop = STEPS - 1
    assert n_blk % 2 == 0 and n_blk > STEPS and n_batch % 2 == 0 and STEPS == 4
    any_spec = pl.BlockSpec(memory_space=pl.ANY)
    hbm_spec = pl.BlockSpec(memory_space=pl.ANY)
    dma = pltpu.SemaphoreType.DMA
    return pl.pallas_call(
        functools.partial(exchange_kernel, n_blk, n_batch),
        out_shape=(
            jax.ShapeDtypeStruct((n_batch, m, jl, chars), BF16),
            jax.ShapeDtypeStruct((hop,) + basis.shape, BF16),
            jax.ShapeDtypeStruct((hop,) + template.shape, BF16),
            jax.ShapeDtypeStruct((hop,) + weights.shape, BF16),
        ),
        in_specs=[hbm_spec] * 4,
        out_specs=(any_spec,) * 4,
        scratch_shapes=[
            pltpu.VMEM((m, jl, chars), BF16),
            dma((n_batch - 1,)), dma((n_batch - 1,)),
            dma((hop + 1, 5)), dma((hop, 5)), dma((hop, 5)), dma((hop, 5)), dma((2,)),
        ],
        compiler_params=pltpu.CompilerParams(
            collective_id=0, has_side_effects=True, vmem_limit_bytes=67043328
        ),
        cost_estimate=pl.CostEstimate(flops=0, bytes_accessed=20 << 20, transcendentals=0),
        name="exchange",
    )(transforms, basis, template, weights)


def skin_kernel(
    co_ref, tr_ref, ba0_ref, te0_ref, we0_ref, ba_ref, te_ref, we_ref, out_ref,
    basis, weights, mixed0, mixed1, mixed2, shaped, poses, coefs,
):
    rows = co_ref.shape[1]
    k = co_ref.shape[0]
    depth = basis.shape[2]
    comps = poses.shape[0]
    joints = weights.shape[1]
    verts = we0_ref.shape[1]
    tiles = verts // LANES
    wide = 2 * LANES

    @pl.when(pl.program_id(0) == 0)
    def _():
        for s in range(STEPS):
            w = (we0_ref[...] if s == 0 else we_ref[s - 1]).astype(F32)
            weights[s] = (w / jnp.sum(w, axis=0, keepdims=True)).astype(BF16)
            te = te0_ref[...] if s == 0 else te_ref[s - 1]
            for e in range(3):
                basis[s, e, :k] = ba0_ref[e] if s == 0 else ba_ref[s - 1, e]
                row = te[e:e + 1].astype(F32)
                pad = jnp.broadcast_to(row, (depth - k, verts))
                first = lax.broadcasted_iota(jnp.int32, (depth - k, verts), 0) == 0
                basis[s, e, k:] = jnp.where(first, pad, 0.0).astype(BF16)

    ones = jnp.where(
        lax.broadcasted_iota(jnp.int32, (depth - k, rows), 0) == 0, 1.0, 0.0
    ).astype(F32)
    padded = jnp.concatenate([co_ref[...].astype(F32), ones], axis=0)
    coefs[...] = padded.T.astype(BF16)
    for m in range(comps):
        parts = [tr_ref[i, m].astype(F32) for i in range(tr_ref.shape[0])]
        poses[m] = jnp.concatenate(parts, axis=0).T.astype(BF16)

    group = tiles * STEPS
    halves = verts // wide
    for s in range(STEPS):
        for n in range(halves):
            for e in range(3):
                shaped[s, n, e] = jnp.dot(
                    coefs[...], basis[s, e, :, n * wide:(n + 1) * wide],
                    preferred_element_type=F32,
                )
    for d, mixed in enumerate((mixed0, mixed1, mixed2)):
        for s in range(STEPS):
            for n in range(halves):
                w = weights[s, :, n * wide:(n + 1) * wide]
                total = jnp.dot(poses[4 * d + 3], w, preferred_element_type=F32)
                for e in range(3):
                    total = total + shaped[s, n, e] * jnp.dot(
                        poses[4 * d + e], w, preferred_element_type=F32
                    )
                for h in range(wide // LANES):
                    at = (n * (wide // LANES) + h) * STEPS + s
                    mixed[pl.ds(at, rows, stride=group), :] = total[:, h * LANES:(h + 1) * LANES]
        out_ref[:, d] = mixed[...].reshape(rows, group, LANES).astype(BF16)


def skin(coefficients, poses, basis, template, weights, basis_in, template_in, weights_in):
    k, chars = coefficients.shape
    n_batch, comps, jl, _ = poses.shape
    verts = weights.shape[1]
    joints = weights.shape[0]
    rows = 2 * LANES if chars % (2 * LANES) == 0 else LANES
    depth = -(-(k + 1) // 8) * 8
    group = (verts // LANES) * STEPS

    def whole(a):
        return pl.BlockSpec(a.shape, lambda i: (0,) * a.ndim)

    out = pl.pallas_call(
        skin_kernel,
        grid=(chars // rows,),
        out_shape=jax.ShapeDtypeStruct((chars, 3, group, LANES), BF16),
        in_specs=[
            pl.BlockSpec((k, rows), lambda i: (0, i)),
            pl.BlockSpec((n_batch, comps, jl, rows), lambda i: (0, 0, 0, i)),
            whole(basis), whole(template), whole(weights),
            whole(basis_in), whole(template_in), whole(weights_in),
        ],
        out_specs=pl.BlockSpec((rows, 3, group, LANES), lambda i: (i, 0, 0, 0)),
        scratch_shapes=[
            pltpu.VMEM((STEPS, 3, depth, verts), BF16),
            pltpu.VMEM((STEPS, joints, verts), BF16),
            pltpu.VMEM((rows * group, LANES), F32),
            pltpu.VMEM((rows * group, LANES), F32),
            pltpu.VMEM((rows * group, LANES), F32),
            pltpu.VMEM((STEPS, verts // (2 * LANES), 3, rows, 2 * LANES), F32),
            pltpu.VMEM((comps, rows, joints), BF16),
            pltpu.VMEM((rows, depth), BF16),
        ],
        compiler_params=pltpu.CompilerParams(
            dimension_semantics=("arbitrary",), vmem_limit_bytes=67043328
        ),
        name="skin",
    )(coefficients, poses, basis, template, weights, basis_in, template_in, weights_in)
    out = out.reshape(chars, 3, verts // LANES, STEPS, LANES)
    return out.transpose(0, 3, 1, 2, 4).reshape(chars, STEPS, 3, verts)


def solution(mesh):
    n_blk, n_batch = mesh.shape["blk"], mesh.shape["batch"]

    def per_device(coefficients, transforms, basis, template, skin_weights):
        basis = jnp.transpose(basis, (1, 0, 2))
        poses, basis_in, template_in, weights_in = exchange(
            n_blk, n_batch, transforms, basis, template, skin_weights
        )
        return skin(
            coefficients, poses, basis, template, skin_weights,
            basis_in, template_in, weights_in,
        )

    in_specs = (
        P(None, ("blk", "batch")),
        P(None, "batch", "blk"),
        P(None, None, "blk"),
        P(None, "blk"),
        P(None, "blk"),
    )
    out_specs = P(("blk", "batch"), None, None, None)
    return jax.shard_map(
        per_device, mesh=mesh, in_specs=in_specs, out_specs=out_specs, check_vma=False
    )
```
